32 devices in a mesh: rep: 1, dp: 32 (over x, y, z, core).
Axes of the slice: x: 2, y: 2, z: 4, core: 2. Of those that a mesh axis runs over, the one named last changes fastest.
Arguments:
- a: bfloat16 [32, 2, 4096, 1152], P(('rep', 'dp'))
- g: bfloat16 [32, 2, 4096, 4608], P(('rep', 'dp'))
Outputs:
- output: bfloat16 [2, 1152, 4608], P('rep')
All inputs are finite; a program needn't handle non-finite values.
Results may differ from the reference program's by a relative error of at most 0.012.
Values are sent between devices in bfloat16 or wider.
A program may use at most 2 GiB of HBM per device.

```python
import jax
import jax.numpy as jnp
from jax import lax

DEVICES = 32
MATRICES = 2
TOKENS = 4096
D = 1152
FF = 4608


def setup_inputs(seed: int = 0, part: int = 0) -> dict:
    ka, kg, ks = (jax.random.fold_in(k, part) for k in jax.random.split(jax.random.key(seed), 3))
    size = 2.0 ** jax.random.uniform(ks, (DEVICES, MATRICES, 1, 1), jnp.float32, -1.0, 1.0)
    a = jax.random.normal(ka, (DEVICES, MATRICES, TOKENS, D), jnp.float32)
    g = size * jax.random.normal(kg, (DEVICES, MATRICES, TOKENS, FF), jnp.float32) * (DEVICES * TOKENS) ** -0.5
    return {"a": a.astype(jnp.bfloat16), "g": g.astype(jnp.bfloat16)}


def reference(a, g):
    def take(so_far, one):
        return so_far + jnp.einsum("ntd,ntf->ndf", *one, preferred_element_type=jnp.float32), None

    return lax.scan(take, jnp.zeros((MATRICES, D, FF), jnp.float32), (a, g))[0].astype(jnp.bfloat16)
```

```python
import functools
import jax
import jax.numpy as jnp
from jax import lax
from jax.experimental import pallas as pl
from jax.experimental.pallas import tpu as pltpu
from jax.sharding import PartitionSpec as P

N, T, D, FF = 2, 4096, 1152, 4608
W = 256
NC = N * FF // W
PER = FF // W
HALF, QUART, EIGHTH = D // 2, D // 4, D // 8
SLAB = 256
NS = T // SLAB
K = 4
KZ = 8
LAG = 2
STAGES = 9
BF, F32 = jnp.bfloat16, jnp.float32


def kernel(a_hbm, g_hbm, res, at, stage, gbuf, acc,
           sd, k1, s1, r1, k2, sz, rz, k3, s3, rx, s4, ry,
           a_sem, g_sem, snd_d, rcv_d, snd_1, rcv_1, snd_z, rcv_z, snd_x, rcv_x, snd_y, rcv_y,
           snd_p, rcv_p, snd_g, rcv_g, snd_h, rcv_h, snd_a, rcv_a, snd_e, rcv_e):
    me = lax.axis_index("dp")
    core, z, y, x = me % 2, (me // 2) % 4, (me // 8) % 2, me // 16
    mid = (z == 1) | (z == 2)
    end = jnp.logical_not(mid)
    to_core = me + 1 - 2 * core
    to_x = me + 16 * (1 - 2 * x)
    to_y = me + 8 * (1 - 2 * y)
    to_z = me + 2 * (1 - 2 * (z % 2))
    to_m = jnp.where(mid, me + 2 * (3 - 2 * z), to_z)
    first = (to_x, to_y)
    second = (to_y, to_x)
    keep = (x, y)
    zq = z // 2

    mine = pl.multiple_of(core * HALF, HALF)
    other = pl.multiple_of((1 - core) * HALF, HALF)

    def rows_h(ab, kept=True):
        h = keep[ab] if kept else 1 - keep[ab]
        return pl.multiple_of(core * HALF + h * QUART, EIGHTH)

    def rows_q(ab, q):
        return pl.multiple_of(core * HALF + keep[ab] * QUART + q * EIGHTH, EIGHTH)

    def remote(src, dst, send, recv, dev):
        return pltpu.make_async_remote_copy(
            src_ref=src, dst_ref=dst, send_sem=send, recv_sem=recv,
            device_id={"dp": dev}, device_id_type=pl.DeviceIdType.MESH)

    def d_copy(c):
        s = c % K
        return remote(sd.at[s], res.at[c, :, pl.ds(other, HALF)], snd_d.at[s], rcv_d.at[s], to_core)

    def d_wait(c):
        s = c % K
        return remote(sd.at[s], res.at[c, :, pl.ds(mine, HALF)], snd_d.at[s], rcv_d.at[s], to_core)

    def c1(c, ab):
        s = c % K
        return remote(s1.at[s, ab], r1.at[s, ab], snd_1.at[s, ab], rcv_1.at[s, ab], first[ab])

    def cz(c, ab):
        s = c % KZ
        return remote(sz.at[s, ab], rz.at[s, ab], snd_z.at[s, ab], rcv_z.at[s, ab], to_z)

    def cx(c, ab):
        s = c % K
        return remote(s3.at[s, ab], rx.at[s, ab], snd_x.at[s, ab], rcv_x.at[s, ab], to_m)

    def cy(c, ab):
        s = c % K
        return remote(s4.at[s, ab], ry.at[s, ab], snd_y.at[s, ab], rcv_y.at[s, ab], second[ab])

    def block(c, ab, start, size):
        return res.at[c, ab, pl.ds(start, size)]

    def back(c, ab, start, size, send, recv, dev):
        ref = block(c, ab, start, size)
        s = c % KZ
        return remote(ref, ref, send.at[s, ab], recv.at[s, ab], dev)

    def cp(c, ab, q):
        return back(c, ab, rows_q(ab, q), EIGHTH, snd_p, rcv_p, to_m)

    def cg(c, ab):
        return back(c, ab, rows_q(ab, zq), EIGHTH, snd_g, rcv_g, to_z)

    def ch(c, ab):
        return back(c, ab, rows_q(ab, 1 - zq), EIGHTH, snd_h, rcv_h, to_z)

    def ca(c, ab, kept):
        return back(c, ab, rows_h(ab, kept), QUART, snd_a, rcv_a, first[ab])

    def ce(c, start):
        ref = res.at[c, :, pl.ds(start, HALF)]
        return remote(ref, ref, snd_e.at[c % K], rcv_e.at[c % K], to_core)

    def run(c, *conds):
        ok = (c >= 0) & (c < NC)
        for one in conds:
            ok = ok & one
        return pl.when(ok)

    def stage1(c):
        @run(c - LAG)
        def _():
            for ab in range(2):
                c1(c - LAG, ab).wait_send()

        @run(c)
        def _():
            s = c % K
            d_wait(c).wait_recv()
            for ab in range(2):
                cols = slice(ab * 128, ab * 128 + 128)
                away, here = rows_h(ab, False), rows_h(ab, True)
                s1[s, ab] = (acc[c % 2, pl.ds(away, QUART), cols]
                             + res[c, ab, pl.ds(away, QUART)].astype(F32)).astype(BF)
                c1(c, ab).start()
                k1[s, ab] = acc[c % 2, pl.ds(here, QUART), cols] + res[c, ab, pl.ds(here, QUART)].astype(F32)

    def stage2(c):
        @run(c - LAG, end)
        def _():
            for ab in range(2):
                cz(c - LAG, ab).wait_send()

        @run(c)
        def _():
            s = c % K
            for ab in range(2):
                c1(c, ab).wait_recv()

                @pl.when(end)
                def _():
                    sz[c % KZ, ab] = (k1[s, ab] + r1[s, ab].astype(F32)).astype(BF)
                    cz(c, ab).start()

                @pl.when(mid)
                def _():
                    k2[s, ab] = k1[s, ab] + r1[s, ab].astype(F32)

    def stage3(c):
        @run(c - LAG, mid)
        def _():
            for ab in range(2):
                cx(c - LAG, ab).wait_send()

        @run(c, mid)
        def _():
            s = c % K
            away = pl.ds(pl.multiple_of((1 - zq) * EIGHTH, EIGHTH), EIGHTH)
            here = pl.ds(pl.multiple_of(zq * EIGHTH, EIGHTH), EIGHTH)
            for ab in range(2):
                cz(c, ab).wait_recv()
                s3[s, ab] = (k2[s, ab, away] + rz[c % KZ, ab, away].astype(F32)).astype(BF)
                cx(c, ab).start()
                k3[s, ab] = k2[s, ab, here] + rz[c % KZ, ab, here].astype(F32)

    def stage4(c):
        @run(c - LAG, mid)
        def _():
            for ab in range(2):
                cy(c - LAG, ab).wait_send()

        @run(c, mid)
        def _():
            s = c % K
            for ab in range(2):
                cx(c, ab).wait_recv()
                s4[s, ab] = (k3[s, ab] + rx[s, ab].astype(F32)).astype(BF)
                cy(c, ab).start()

    def stage5(c):
        @run(c - LAG, mid)
        def _():
            for ab in range(2):
                cp(c - LAG, ab, zq).wait_send()
                cg(c - LAG, ab).wait_send()

        @run(c, mid)
        def _():
            s = c % K
            for ab in range(2):
                cy(c, ab).wait_recv()
                res[c, ab, pl.ds(rows_q(ab, zq), EIGHTH)] = (
                    s4[s, ab].astype(F32) + ry[s, ab].astype(F32)).astype(BF)
                cp(c, ab, zq).start()
                cg(c, ab).start()

    def stage6(c):
        @run(c - LAG, mid)
        def _():
            for ab in range(2):
                ch(c - LAG, ab).wait_send()
                ca(c - LAG, ab, True).wait_send()

        @run(c, mid)
        def _():
            for ab in range(2):
                cp(c, ab, 1 - zq).wait_recv()
                ch(c, ab).start()
                ca(c, ab, True).start()

    def stage7(c):
        @run(c - LAG, end)
        def _():
            for ab in range(2):
                ca(c - LAG, ab, True).wait_send()

        @run(c, end)
        def _():
            for ab in range(2):
                cg(c, ab).wait_recv()
                ch(c, ab).wait_recv()
                ca(c, ab, True).start()

    def stage8(c):
        @run(c - LAG)
        def _():
            ce(c - LAG, mine).wait_send()

        @run(c)
        def _():
            for ab in range(2):
                ca(c, ab, False).wait_recv()
            ce(c, mine).start()

    def stage9(c):
        @run(c)
        def _():
            ce(c, other).wait_recv()

    def g_copy(c):
        cols = pl.ds(pl.multiple_of((c % PER) * W, W), W)
        return pltpu.make_async_copy(g_hbm.at[c // PER, :, cols], gbuf.at[c % 2], g_sem.at[c % 2])

    def a_copy(i):
        return pltpu.make_async_copy(
            a_hbm.at[i // NS, pl.ds(pl.multiple_of((i % NS) * SLAB, SLAB), SLAB)],
            stage.at[i % K], a_sem.at[i % K])

    def transpose(i):
        a_copy(i).wait()
        at[i // NS, :, pl.ds(pl.multiple_of((i % NS) * SLAB, SLAB), SLAB)] = stage[i % K].T

        @pl.when(i + K < 2 * NS)
        def _():
            a_copy(i + K).start()

    def matmul(c):
        @run(c - LAG)
        def _():
            d_copy(c - LAG).wait_send()

        @run(c)
        def _():
            g_copy(c).wait()

            @pl.when(c + 1 < NC)
            def _():
                g_copy(c + 1).start()

            acc[c % 2] = jnp.dot(at[c // PER], gbuf[c % 2], preferred_element_type=F32)
            for ab in range(2):
                sd[c % K, ab] = acc[c % 2, pl.ds(other, HALF), ab * 128:ab * 128 + 128].astype(BF)
            d_copy(c).start()

        @pl.when(c < NS)
        def _():
            transpose(NS + c)

    for i in range(K):
        a_copy(i).start()
    g_copy(0).start()
    barrier = pltpu.get_barrier_semaphore()
    for dev in (to_core, to_x, to_y, to_z):
        pl.semaphore_signal(barrier, inc=1, device_id={"dp": dev}, device_id_type=pl.DeviceIdType.MESH)

    @pl.when(mid)
    def _():
        pl.semaphore_signal(barrier, inc=1, device_id={"dp": to_m}, device_id_type=pl.DeviceIdType.MESH)
        pl.semaphore_wait(barrier, 5)

    @pl.when(end)
    def _():
        pl.semaphore_wait(barrier, 4)

    @pl.loop(0, NS)
    def _(i):
        transpose(i)

    @pl.loop(0, NC + STAGES + LAG)
    def _(t):
        stage9(t - 9)
        stage8(t - 8)
        stage7(t - 7)
        stage6(t - 6)
        stage5(t - 5)
        stage4(t - 4)
        stage3(t - 3)
        stage2(t - 2)
        stage1(t - 1)
        matmul(t)


def place_kernel(res, out, sem):
    def copy(i):
        c, ab = i // 2, i % 2
        cols = pl.ds(pl.multiple_of((c % PER) * W + ab * 128, 128), 128)
        return pltpu.make_async_copy(res.at[c, ab], out.at[c // PER, :, cols], sem)

    @pl.loop(0, 2 * NC)
    def _(i):
        copy(i).start()

    pltpu.make_async_copy(res, res, sem).wait()


def total(a, g):
    dma = pltpu.SemaphoreType.DMA
    res = pl.pallas_call(
        kernel,
        out_shape=pltpu.VMEM((NC, 2, D, 128), BF),
        in_specs=[pl.BlockSpec(memory_space=pl.ANY)] * 2,
        out_specs=pl.BlockSpec(memory_space=pltpu.VMEM),
        scratch_shapes=[
            pltpu.VMEM((N, D, T), BF),
            pltpu.VMEM((K, SLAB, D), BF),
            pltpu.VMEM((2, T, W), BF),
            pltpu.VMEM((2, D, W), F32),
            pltpu.VMEM((K, 2, HALF, 128), BF),
            pltpu.VMEM((K, 2, QUART, 128), F32),
            pltpu.VMEM((K, 2, QUART, 128), BF),
            pltpu.VMEM((K, 2, QUART, 128), BF),
            pltpu.VMEM((K, 2, QUART, 128), F32),
            pltpu.VMEM((KZ, 2, QUART, 128), BF),
            pltpu.VMEM((KZ, 2, QUART, 128), BF),
            pltpu.VMEM((K, 2, EIGHTH, 128), F32),
            pltpu.VMEM((K, 2, EIGHTH, 128), BF),
            pltpu.VMEM((K, 2, EIGHTH, 128), BF),
            pltpu.VMEM((K, 2, EIGHTH, 128), BF),
            pltpu.VMEM((K, 2, EIGHTH, 128), BF),
            dma((K,)), dma((2,)),
            dma((K,)), dma((K,)),
        ] + [dma((K, 2))] * 2 + [dma((KZ, 2))] * 2 + [dma((K, 2))] * 4 + [dma((KZ, 2))] * 8 + [dma((K,)), dma((K,))],
        compiler_params=pltpu.CompilerParams(
            collective_id=0, has_side_effects=True, vmem_limit_bytes=VL),
        name="sum_tiles",
    )(a, g)
    return pl.pallas_call(
        place_kernel,
        out_shape=jax.ShapeDtypeStruct((N, D, FF), BF),
        in_specs=[pl.BlockSpec(memory_space=pltpu.VMEM)],
        out_specs=pl.BlockSpec(memory_space=pl.ANY),
        scratch_shapes=[pltpu.SemaphoreType.DMA],
        compiler_params=pltpu.CompilerParams(vmem_limit_bytes=VL2),
        name="place",
    )(res)


VL = 42 * 2**20
VL2 = 30 * 2**20


def solution(mesh):
    def body(a, g):
        return total(a[0], g[0])

    return jax.shard_map(body, mesh=mesh, in_specs=(P(("rep", "dp")), P(("rep", "dp"))),
                         out_specs=P("rep"), check_vma=False)
```

```python
import jax
import jax.numpy as jnp
from jax import lax
from jax.experimental import pallas as pl
from jax.experimental.pallas import tpu as pltpu
from jax.sharding import PartitionSpec as P

N, T, D, FF = 2, 4096, 1152, 4608
W = 256
NC = N * FF // W
PER = FF // W
HALF, QUART = D // 2, D // 4
OUT, IN = 64, 80
SIDE = OUT + IN
SLAB = 256
NS = T // SLAB
K, KR = 4, 8
LAG = 2
AS = 3
OFF = {1: 2, 2: 3, 3: 4, 4: 6, 5: 9, 6: 9, 7: 10, 8: 11, "A": 15, "B": 22}
ORDER = (5, 1, "A", "M", 4, 7, 8, 3, 2, "B", 6)
BF, F32 = jnp.bfloat16, jnp.float32
DMA = pltpu.SemaphoreType.DMA

BUFFERS = dict(
    at=pltpu.VMEM((N, D, T), BF),
    stage=pltpu.VMEM((AS, SLAB, D), BF),
    gbuf=pltpu.VMEM((2, T, W), BF),
    acc=pltpu.VMEM((2, D, W), F32),
    sd=pltpu.VMEM((K, 2, HALF, 128), BF),
    k1=pltpu.VMEM((K, 2, QUART, 128), F32),
    s1=pltpu.VMEM((K, 2, QUART, 128), BF),
    r1=pltpu.VMEM((KR, 2, QUART, 128), BF),
    k2=pltpu.VMEM((K, 2, QUART, 128), F32),
    sz=pltpu.VMEM((K, 2, QUART - OUT, 128), BF),
    rz=pltpu.VMEM((KR, 2, QUART - OUT, 128), BF),
    ke=pltpu.VMEM((KR, 2, OUT, 128), F32),
    k3=pltpu.VMEM((K, 2, SIDE, 128), F32),
    s3=pltpu.VMEM((K, 2, SIDE, 128), BF),
    rx=pltpu.VMEM((KR, 2, SIDE, 128), BF),
    sc=pltpu.VMEM((K, 2, OUT, 128), BF),
    rc=pltpu.VMEM((KR, 2, OUT, 128), BF),
    s4=pltpu.VMEM((KR, 2, IN, 128), BF),
    ry=pltpu.VMEM((KR, 2, IN, 128), BF),
)
LINKS = ("1", "z", "x", "c", "y", "g1", "g2", "p1", "p0", "q0", "a")
SEMS = dict(a_sem=DMA((AS,)), g_sem=DMA((2,)),
            snd_d=DMA((K,)), rcv_d=DMA((KR,)), snd_e=DMA((K,)), rcv_e=DMA((NC,)))
for link in LINKS:
    SEMS["snd_" + link] = DMA((K, 2))
    SEMS["rcv_" + link] = DMA((KR if link in ("1", "z", "x", "c", "y") else NC, 2))
SCRATCH = {**BUFFERS, **SEMS}


def kernel(a_hbm, g_hbm, res, *scratch):
    r = dict(zip(SCRATCH, scratch))
    me = lax.axis_index("dp")
    core, z, y, x = me % 2, (me // 2) % 4, (me // 8) % 2, me // 16
    mid = (z == 1) | (z == 2)
    end = jnp.logical_not(mid)
    to_core = me + 1 - 2 * core
    to_x = me + 16 * (1 - 2 * x)
    to_y = me + 8 * (1 - 2 * y)
    to_z = me + 2 * (1 - 2 * (z % 2))
    to_m = jnp.where(mid, me + 2 * (3 - 2 * z), to_z)
    first = (to_x, to_y)
    second = (to_y, to_x)
    keep = (x, y)
    side = z // 2

    def aligned(v):
        return pl.multiple_of(v, 16)

    mine = aligned(core * HALF)
    other = aligned((1 - core) * HALF)
    out_at = side * (QUART - OUT)
    in_at = OUT + side * IN
    far_at = (1 - side) * SIDE
    up_at = (1 - side) * OUT

    def quarter(ab, kept=True):
        return aligned(core * HALF + (keep[ab] if kept else 1 - keep[ab]) * QUART)

    def rows(v, size):
        return pl.ds(aligned(v), size)

    def remote(src, dst, link, c, ab, dev):
        snd, rcv = r["snd_" + link], r["rcv_" + link]
        ks, kr = snd.shape[0], rcv.shape[0]
        at = () if ab is None else (ab,)
        return pltpu.make_async_remote_copy(
            src_ref=src, dst_ref=dst, send_sem=snd.at[(c % ks,) + at], recv_sem=rcv.at[(c % kr,) + at],
            device_id={"dp": dev}, device_id_type=pl.DeviceIdType.MESH)

    def d_copy(c, start):
        return remote(r["sd"].at[c % K], res.at[c, :, pl.ds(start, HALF)], "d", c, None, to_core)

    def c1(c, ab):
        return remote(r["s1"].at[c % K, ab], r["r1"].at[c % KR, ab], "1", c, ab, first[ab])

    def cz(c, ab):
        return remote(r["sz"].at[c % K, ab], r["rz"].at[c % KR, ab], "z", c, ab, to_z)

    def cx(c, ab):
        return remote(r["s3"].at[c % K, ab], r["rx"].at[c % KR, ab], "x", c, ab, to_m)

    def cc(c, ab):
        return remote(r["sc"].at[c % K, ab], r["rc"].at[c % KR, ab], "c", c, ab, to_z)

    def cy(c, ab, size):
        return remote(r["s4"].at[c % KR, ab, pl.ds(0, size)], r["ry"].at[c % KR, ab, pl.ds(0, size)],
                      "y", c, ab, second[ab])

    def part(link, c, ab, v, size, dev):
        ref = res.at[c, ab, rows(quarter(ab) + v, size)]
        return remote(ref, ref, link, c, ab, dev)

    def g1(c, ab):
        return part("g1", c, ab, in_at, IN, to_z)

    def g2(c, ab):
        return part("g2", c, ab, far_at, SIDE, to_z)

    def p1(c, ab, s=None):
        return part("p1", c, ab, in_at if s is None else OUT + s * IN, IN, to_m)

    def p0(c, ab, s=None):
        return part("p0", c, ab, out_at if s is None else s * (QUART - OUT), OUT, to_m)

    def q0(c, ab):
        return part("q0", c, ab, out_at, OUT, to_z)

    def ca(c, ab, kept=True):
        ref = res.at[c, ab, pl.ds(quarter(ab, kept), QUART)]
        return remote(ref, ref, "a", c, ab, first[ab])

    def ce(c, start):
        ref = res.at[c, :, pl.ds(start, HALF)]
        return remote(ref, ref, "e", c, None, to_core)

    sent = []

    def settle(c, where, *copies):
        sent.append((where, copies))

        @pl.when((c >= LAG) & (c < NC) & where)
        def _():
            for copy in copies:
                for ab in range(2):
                    copy(c - LAG, ab).wait_send()

    def run(c, where):
        return pl.when((c >= 0) & (c < NC) & where)

    def f32(ref):
        return ref.astype(F32)

    def stage1(c):
        settle(c, True, c1)

        @run(c, True)
        def _():
            d_copy(c, mine).wait_recv()
            for ab in range(2):
                cols = slice(ab * 128, ab * 128 + 128)
                away, here = pl.ds(quarter(ab, False), QUART), pl.ds(quarter(ab), QUART)
                r["s1"][c % K, ab] = (r["acc"][c % 2, away, cols] + f32(res[c, ab, away])).astype(BF)
                c1(c, ab).start()
                r["k1"][c % K, ab] = r["acc"][c % 2, here, cols] + f32(res[c, ab, here])

    def stage2(c):
        settle(c, end, cz)

        @run(c, True)
        def _():
            for ab in range(2):
                c1(c, ab).wait_recv()

                @pl.when(end)
                def _():
                    up, own = rows(up_at, QUART - OUT), rows(out_at, OUT)
                    r["sz"][c % K, ab] = (r["k1"][c % K, ab, up] + f32(r["r1"][c % KR, ab, up])).astype(BF)
                    cz(c, ab).start()
                    r["ke"][c % KR, ab] = r["k1"][c % K, ab, own] + f32(r["r1"][c % KR, ab, own])

                @pl.when(mid)
                def _():
                    r["k2"][c % K, ab] = r["k1"][c % K, ab] + f32(r["r1"][c % KR, ab])

    def stage3(c):
        settle(c, mid, cx)

        @run(c, mid)
        def _():
            for ab in range(2):
                cz(c, ab).wait_recv()
                rz, k2, k3 = r["rz"], r["k2"], r["k3"]
                r["s3"][c % K, ab] = (k2[c % K, ab, rows(far_at, SIDE)]
                                      + f32(rz[c % KR, ab, rows((1 - side) * IN, SIDE)])).astype(BF)
                cx(c, ab).start()
                k3[c % K, ab, 0:IN] = k2[c % K, ab, rows(in_at, IN)] + f32(rz[c % KR, ab, rows(side * SIDE, IN)])
                k3[c % K, ab, IN:SIDE] = k2[c % K, ab, rows(out_at, OUT)]

    def stage4(c):
        settle(c, mid, cc, lambda c, ab: cy(c, ab, IN))

        @run(c, mid)
        def _():
            for ab in range(2):
                cx(c, ab).wait_recv()
                k3, rx = r["k3"], r["rx"]
                r["sc"][c % K, ab] = (k3[c % K, ab, IN:SIDE]
                                      + f32(rx[c % KR, ab, rows(side * IN, OUT)])).astype(BF)
                cc(c, ab).start()
                r["s4"][c % KR, ab] = (k3[c % K, ab, 0:IN]
                                       + f32(rx[c % KR, ab, rows((1 - side) * OUT, IN)])).astype(BF)
                cy(c, ab, IN).start()

    def stage5(c):
        settle(c, end, lambda c, ab: cy(c, ab, OUT))

        @run(c, end)
        def _():
            for ab in range(2):
                cc(c, ab).wait_recv()
                r["s4"][c % KR, ab, 0:OUT] = (r["ke"][c % KR, ab] + f32(r["rc"][c % KR, ab])).astype(BF)
                cy(c, ab, OUT).start()

    def stage6(c):
        settle(c, mid, g1, p1)
        settle(c, end, q0)

        def last(ab, v, size):
            cy(c, ab, size).wait_recv()
            res[c, ab, rows(quarter(ab) + v, size)] = (
                f32(r["s4"][c % KR, ab, 0:size]) + f32(r["ry"][c % KR, ab, 0:size])).astype(BF)

        @run(c, mid)
        def _():
            for ab in range(2):
                last(ab, in_at, IN)
                p1(c, ab).start()
                g1(c, ab).start()

        @run(c, end)
        def _():
            for ab in range(2):
                last(ab, out_at, OUT)
                q0(c, ab).start()

    def stage7(c):
        settle(c, mid, p0)

        @run(c, mid)
        def _():
            for ab in range(2):
                q0(c, ab).wait_recv()
                p0(c, ab).start()

    def stage8(c):
        settle(c, mid, g2)

        @run(c, mid)
        def _():
            for ab in range(2):
                p1(c, ab, 1 - side).wait_recv()
                p0(c, ab, 1 - side).wait_recv()
                g2(c, ab).start()

    def stage_a(c):
        settle(c, True, ca)

        @run(c, True)
        def _():
            for ab in range(2):
                @pl.when(end)
                def _():
                    g1(c, ab).wait_recv()
                    g2(c, ab).wait_recv()

                ca(c, ab).start()

    def stage_b(c):
        @pl.when((c >= LAG) & (c < NC))
        def _():
            ce(c - LAG, mine).wait_send()

        @run(c, True)
        def _():
            for ab in range(2):
                ca(c, ab, False).wait_recv()
            ce(c, mine).start()

    def g_copy(c):
        cols = pl.ds(pl.multiple_of((c % PER) * W, W), W)
        return pltpu.make_async_copy(g_hbm.at[c // PER, :, cols], r["gbuf"].at[c % 2], r["g_sem"].at[c % 2])

    def a_copy(i):
        return pltpu.make_async_copy(
            a_hbm.at[i // NS, pl.ds(pl.multiple_of((i % NS) * SLAB, SLAB), SLAB)],
            r["stage"].at[i % AS], r["a_sem"].at[i % AS])

    def transpose(i):
        a_copy(i).wait()
        r["at"][i // NS, :, pl.ds(pl.multiple_of((i % NS) * SLAB, SLAB), SLAB)] = r["stage"][i % AS].T

        @pl.when(i + AS < 2 * NS)
        def _():
            a_copy(i + AS).start()

    def matmul(c):
        @pl.when((c >= LAG) & (c < NC))
        def _():
            d_copy(c - LAG, other).wait_send()

        @run(c, True)
        def _():
            g_copy(c).wait()

            @pl.when(c + 1 < NC)
            def _():
                g_copy(c + 1).start()

            r["acc"][c % 2] = jnp.dot(r["at"][c // PER], r["gbuf"][c % 2], preferred_element_type=F32)
            for ab in range(2):
                cols = slice(ab * 128, ab * 128 + 128)
                r["sd"][c % K, ab] = r["acc"][c % 2, pl.ds(other, HALF), cols].astype(BF)
            d_copy(c, other).start()

        @pl.when(c < NS)
        def _():
            transpose(NS + c)

    for i in range(AS):
        a_copy(i).start()
    g_copy(0).start()
    barrier = pltpu.get_barrier_semaphore()

    def greet(dev):
        pl.semaphore_signal(barrier, inc=1, device_id={"dp": dev}, device_id_type=pl.DeviceIdType.MESH)

    for dev in (to_core, to_x, to_y, to_z):
        greet(dev)

    @pl.when(mid)
    def _():
        greet(to_m)
        pl.semaphore_wait(barrier, 5)

    @pl.when(end)
    def _():
        pl.semaphore_wait(barrier, 4)

    @pl.loop(0, NS)
    def _(i):
        transpose(i)

    steps = {1: stage1, 2: stage2, 3: stage3, 4: stage4, 5: stage5, 6: stage6, 7: stage7, 8: stage8,
             "A": stage_a, "B": stage_b, "M": matmul}

    @pl.loop(0, NC + max(OFF.values()))
    def _(t):
        for name in ORDER:
            steps[name](t - OFF.get(name, 0))

    for c in range(NC - LAG, NC):
        for where, copies in sent:
            @pl.when(where)
            def _():
                for copy in copies:
                    for ab in range(2):
                        copy(c, ab).wait_send()
        d_copy(c, other).wait_send()
        ce(c, mine).wait_send()

    @pl.loop(0, NC)
    def _(c):
        ce(c, other).wait_recv()


def place_kernel(res, out, sem):
    def copy(i):
        c, ab = i // 2, i % 2
        cols = pl.ds(pl.multiple_of((c % PER) * W + ab * 128, 128), 128)
        return pltpu.make_async_copy(res.at[c, ab], out.at[c // PER, :, cols], sem)

    @pl.loop(0, 2 * NC)
    def _(i):
        copy(i).start()

    pltpu.make_async_copy(res, res, sem).wait()


def total(a, g):
    res = pl.pallas_call(
        kernel,
        out_shape=pltpu.VMEM((NC, 2, D, 128), BF),
        in_specs=[pl.BlockSpec(memory_space=pl.ANY)] * 2,
        out_specs=pl.BlockSpec(memory_space=pltpu.VMEM),
        scratch_shapes=list(SCRATCH.values()),
        compiler_params=pltpu.CompilerParams(
            collective_id=0, has_side_effects=True, vmem_limit_bytes=42 * 2**20),
        name="sum_tiles",
    )(a, g)
    return pl.pallas_call(
        place_kernel,
        out_shape=jax.ShapeDtypeStruct((N, D, FF), BF),
        in_specs=[pl.BlockSpec(memory_space=pltpu.VMEM)],
        out_specs=pl.BlockSpec(memory_space=pl.ANY),
        scratch_shapes=[pltpu.SemaphoreType.DMA],
        compiler_params=pltpu.CompilerParams(vmem_limit_bytes=30 * 2**20),
        name="place",
    )(res)


def solution(mesh):
    def body(a, g):
        return total(a[0], g[0])

    return jax.shard_map(body, mesh=mesh, in_specs=(P(("rep", "dp")), P(("rep", "dp"))),
                         out_specs=P("rep"), check_vma=False)
```

```python
import jax
import jax.numpy as jnp
from jax import lax
from jax.experimental import pallas as pl
from jax.experimental.pallas import tpu as pltpu
from jax.sharding import PartitionSpec as P

N, T, D, FF = 2, 4096, 1152, 4608
W = 256
NC = N * FF // W
PER = FF // W
HALF, QUART = D // 2, D // 4
OUT, IN = 64, 80
SIDE = OUT + IN
SLAB = 256
NS = T // SLAB
K, KR = 4, 8
LAG = 2
AS = 3
OFF = {1: 1, 2: 3, 3: 4, 4: 5, 5: 7, 6: 8, 7: 9, 8: 10, "A": 13, "B": 20}
ORDER = (5, "A", 7, 8, 6, "B", 2, "M0", 3, 1, 4, "M1")
BF, F32 = jnp.bfloat16, jnp.float32
DMA = pltpu.SemaphoreType.DMA

BUFFERS = dict(
    at=pltpu.VMEM((N, D, T), BF),
    stage=pltpu.VMEM((AS, SLAB, D), BF),
    gbuf=pltpu.VMEM((2, T, W), BF),
    acc=pltpu.VMEM((3, HALF, W), F32),
    sd=pltpu.VMEM((K, 2, HALF, 128), BF),
    k1=pltpu.VMEM((K, 2, QUART, 128), F32),
    s1=pltpu.VMEM((K, 2, QUART, 128), BF),
    r1=pltpu.VMEM((KR, 2, QUART, 128), BF),
    k2=pltpu.VMEM((K, 2, QUART, 128), F32),
    sz=pltpu.VMEM((K, 2, QUART - OUT, 128), BF),
    rz=pltpu.VMEM((KR, 2, QUART - OUT, 128), BF),
    ke=pltpu.VMEM((KR, 2, OUT, 128), F32),
    k3=pltpu.VMEM((K, 2, SIDE, 128), F32),
    s3=pltpu.VMEM((K, 2, SIDE, 128), BF),
    rx=pltpu.VMEM((KR, 2, SIDE, 128), BF),
    sc=pltpu.VMEM((K, 2, OUT, 128), BF),
    rc=pltpu.VMEM((KR, 2, OUT, 128), BF),
    s4=pltpu.VMEM((KR, 2, IN, 128), BF),
    ry=pltpu.VMEM((KR, 2, IN, 128), BF),
)
LINKS = ("1", "z", "x", "c", "y", "g1", "g2", "p1", "p0", "q0", "a")
SEMS = dict(a_sem=DMA((AS,)), g_sem=DMA((2,)),
            snd_d=DMA((K,)), rcv_d=DMA((KR,)), snd_e=DMA((K,)), rcv_e=DMA((NC,)))
for link in LINKS:
    SEMS["snd_" + link] = DMA((K, 2))
    SEMS["rcv_" + link] = DMA((KR if link in ("1", "z", "x", "c", "y") else NC, 2))
SCRATCH = {**BUFFERS, **SEMS}


def kernel(a_hbm, g_hbm, res, *scratch):
    r = dict(zip(SCRATCH, scratch))
    me = lax.axis_index("dp")
    core, z, y, x = me % 2, (me // 2) % 4, (me // 8) % 2, me // 16
    mid = (z == 1) | (z == 2)
    end = jnp.logical_not(mid)
    to_core = me + 1 - 2 * core
    to_x = me + 16 * (1 - 2 * x)
    to_y = me + 8 * (1 - 2 * y)
    to_z = me + 2 * (1 - 2 * (z % 2))
    to_m = jnp.where(mid, me + 2 * (3 - 2 * z), to_z)
    first = (to_x, to_y)
    second = (to_y, to_x)
    keep = (x, y)
    side = z // 2

    def aligned(v):
        return pl.multiple_of(v, 16)

    mine = aligned(core * HALF)
    other = aligned((1 - core) * HALF)
    out_at = side * (QUART - OUT)
    in_at = OUT + side * IN
    far_at = (1 - side) * SIDE
    up_at = (1 - side) * OUT

    def quarter(ab, kept=True):
        return aligned(core * HALF + (keep[ab] if kept else 1 - keep[ab]) * QUART)

    def rows(v, size):
        return pl.ds(aligned(v), size)

    def remote(src, dst, link, c, ab, dev):
        snd, rcv = r["snd_" + link], r["rcv_" + link]
        ks, kr = snd.shape[0], rcv.shape[0]
        at = () if ab is None else (ab,)
        return pltpu.make_async_remote_copy(
            src_ref=src, dst_ref=dst, send_sem=snd.at[(c % ks,) + at], recv_sem=rcv.at[(c % kr,) + at],
            device_id={"dp": dev}, device_id_type=pl.DeviceIdType.MESH)

    def d_copy(c, start):
        return remote(r["sd"].at[c % K], res.at[c, :, pl.ds(start, HALF)], "d", c, None, to_core)

    def c1(c, ab):
        return remote(r["s1"].at[c % K, ab], r["r1"].at[c % KR, ab], "1", c, ab, first[ab])

    def cz(c, ab):
        return remote(r["sz"].at[c % K, ab], r["rz"].at[c % KR, ab], "z", c, ab, to_z)

    def cx(c, ab):
        return remote(r["s3"].at[c % K, ab], r["rx"].at[c % KR, ab], "x", c, ab, to_m)

    def cc(c, ab):
        return remote(r["sc"].at[c % K, ab], r["rc"].at[c % KR, ab], "c", c, ab, to_z)

    def cy(c, ab, size):
        return remote(r["s4"].at[c % KR, ab, pl.ds(0, size)], r["ry"].at[c % KR, ab, pl.ds(0, size)],
                      "y", c, ab, second[ab])

    def part(link, c, ab, v, size, dev):
        ref = res.at[c, ab, rows(quarter(ab) + v, size)]
        return remote(ref, ref, link, c, ab, dev)

    def g1(c, ab):
        return part("g1", c, ab, in_at, IN, to_z)

    def g2(c, ab):
        return part("g2", c, ab, far_at, SIDE, to_z)

    def p1(c, ab, s=None):
        return part("p1", c, ab, in_at if s is None else OUT + s * IN, IN, to_m)

    def p0(c, ab, s=None):
        return part("p0", c, ab, out_at if s is None else s * (QUART - OUT), OUT, to_m)

    def q0(c, ab):
        return part("q0", c, ab, out_at, OUT, to_z)

    def ca(c, ab, kept=True):
        ref = res.at[c, ab, pl.ds(quarter(ab, kept), QUART)]
        return remote(ref, ref, "a", c, ab, first[ab])

    def ce(c, start):
        ref = res.at[c, :, pl.ds(start, HALF)]
        return remote(ref, ref, "e", c, None, to_core)

    sent = []

    def settle(c, where, *copies):
        sent.append((where, copies))

        @pl.when((c >= LAG) & (c < NC) & where)
        def _():
            for copy in copies:
                for ab in range(2):
                    copy(c - LAG, ab).wait_send()

    def run(c, where):
        return pl.when((c >= 0) & (c < NC) & where)

    def f32(ref):
        return ref.astype(F32)

    def stage1(c):
        settle(c, True, c1)

        @run(c, True)
        def _():
            d_copy(c, mine).wait_recv()
            for ab in range(2):
                cols = slice(ab * 128, ab * 128 + 128)
                h = keep[ab]
                away, here = rows((1 - h) * QUART, QUART), rows(h * QUART, QUART)
                r["s1"][c % K, ab] = (r["acc"][c % 3, away, cols]
                                      + f32(res[c, ab, pl.ds(quarter(ab, False), QUART)])).astype(BF)
                c1(c, ab).start()
                r["k1"][c % K, ab] = r["acc"][c % 3, here, cols] + f32(res[c, ab, pl.ds(quarter(ab), QUART)])

    def stage2(c):
        settle(c, end, cz)

        @run(c, True)
        def _():
            for ab in range(2):
                c1(c, ab).wait_recv()

                @pl.when(end)
                def _():
                    up, own = rows(up_at, QUART - OUT), rows(out_at, OUT)
                    r["sz"][c % K, ab] = (r["k1"][c % K, ab, up] + f32(r["r1"][c % KR, ab, up])).astype(BF)
                    cz(c, ab).start()
                    r["ke"][c % KR, ab] = r["k1"][c % K, ab, own] + f32(r["r1"][c % KR, ab, own])

                @pl.when(mid)
                def _():
                    r["k2"][c % K, ab] = r["k1"][c % K, ab] + f32(r["r1"][c % KR, ab])

    def stage3(c):
        settle(c, mid, cx)

        @run(c, mid)
        def _():
            for ab in range(2):
                cz(c, ab).wait_recv()
                rz, k2, k3 = r["rz"], r["k2"], r["k3"]
                r["s3"][c % K, ab] = (k2[c % K, ab, rows(far_at, SIDE)]
                                      + f32(rz[c % KR, ab, rows((1 - side) * IN, SIDE)])).astype(BF)
                cx(c, ab).start()
                k3[c % K, ab, 0:IN] = k2[c % K, ab, rows(in_at, IN)] + f32(rz[c % KR, ab, rows(side * SIDE, IN)])
                k3[c % K, ab, IN:SIDE] = k2[c % K, ab, rows(out_at, OUT)]

    def stage4(c):
        settle(c, mid, cc, lambda c, ab: cy(c, ab, IN))

        @run(c, mid)
        def _():
            for ab in range(2):
                cx(c, ab).wait_recv()
                k3, rx = r["k3"], r["rx"]
                r["sc"][c % K, ab] = (k3[c % K, ab, IN:SIDE]
                                      + f32(rx[c % KR, ab, rows(side * IN, OUT)])).astype(BF)
                cc(c, ab).start()
                r["s4"][c % KR, ab] = (k3[c % K, ab, 0:IN]
                                       + f32(rx[c % KR, ab, rows((1 - side) * OUT, IN)])).astype(BF)
                cy(c, ab, IN).start()

    def stage5(c):
        settle(c, end, lambda c, ab: cy(c, ab, OUT))

        @run(c, end)
        def _():
            for ab in range(2):
                cc(c, ab).wait_recv()
                r["s4"][c % KR, ab, 0:OUT] = (r["ke"][c % KR, ab] + f32(r["rc"][c % KR, ab])).astype(BF)
                cy(c, ab, OUT).start()

    def stage6(c):
        settle(c, mid, g1, p1)
        settle(c, end, q0)

        def last(ab, v, size):
            cy(c, ab, size).wait_recv()
            res[c, ab, rows(quarter(ab) + v, size)] = (
                f32(r["s4"][c % KR, ab, 0:size]) + f32(r["ry"][c % KR, ab, 0:size])).astype(BF)

        @run(c, mid)
        def _():
            for ab in range(2):
                last(ab, in_at, IN)
                p1(c, ab).start()
                g1(c, ab).start()

        @run(c, end)
        def _():
            for ab in range(2):
                last(ab, out_at, OUT)
                q0(c, ab).start()

    def stage7(c):
        settle(c, mid, p0)

        @run(c, mid)
        def _():
            for ab in range(2):
                q0(c, ab).wait_recv()
                p0(c, ab).start()

    def stage8(c):
        settle(c, mid, g2)

        @run(c, mid)
        def _():
            for ab in range(2):
                p1(c, ab, 1 - side).wait_recv()
                p0(c, ab, 1 - side).wait_recv()
                g2(c, ab).start()

    def stage_a(c):
        settle(c, True, ca)

        @run(c, True)
        def _():
            for ab in range(2):
                @pl.when(end)
                def _():
                    g1(c, ab).wait_recv()
                    g2(c, ab).wait_recv()

                ca(c, ab).start()

    def stage_b(c):
        @pl.when((c >= LAG) & (c < NC))
        def _():
            ce(c - LAG, mine).wait_send()

        @run(c, True)
        def _():
            for ab in range(2):
                ca(c, ab, False).wait_recv()
            ce(c, mine).start()

    def g_copy(c):
        cols = pl.ds(pl.multiple_of((c % PER) * W, W), W)
        return pltpu.make_async_copy(g_hbm.at[c // PER, :, cols], r["gbuf"].at[c % 2], r["g_sem"].at[c % 2])

    def a_copy(i):
        return pltpu.make_async_copy(
            a_hbm.at[i // NS, pl.ds(pl.multiple_of((i % NS) * SLAB, SLAB), SLAB)],
            r["stage"].at[i % AS], r["a_sem"].at[i % AS])

    def transpose(i):
        a_copy(i).wait()
        r["at"][i // NS, :, pl.ds(pl.multiple_of((i % NS) * SLAB, SLAB), SLAB)] = r["stage"][i % AS].T

        @pl.when(i + AS < 2 * NS)
        def _():
            a_copy(i + AS).start()

    def product(c, start):
        return jnp.dot(r["at"][c // PER, pl.ds(start, HALF)], r["gbuf"][c % 2], preferred_element_type=F32)

    def matmul0(c):
        @pl.when((c >= LAG) & (c < NC))
        def _():
            d_copy(c - LAG, other).wait_send()

        @run(c, True)
        def _():
            g_copy(c).wait()

            @pl.when(c + 1 < NC)
            def _():
                g_copy(c + 1).start()

            out = product(c, other).astype(BF)
            for ab in range(2):
                r["sd"][c % K, ab] = out[:, ab * 128:ab * 128 + 128]
            d_copy(c, other).start()

    def matmul1(c):
        @run(c, True)
        def _():
            r["acc"][c % 3] = product(c, mine)

        @pl.when(c < NS)
        def _():
            transpose(NS + c)

    for i in range(AS):
        a_copy(i).start()
    g_copy(0).start()
    barrier = pltpu.get_barrier_semaphore()

    def greet(dev):
        pl.semaphore_signal(barrier, inc=1, device_id={"dp": dev}, device_id_type=pl.DeviceIdType.MESH)

    for dev in (to_core, to_x, to_y, to_z):
        greet(dev)

    @pl.when(mid)
    def _():
        greet(to_m)
        pl.semaphore_wait(barrier, 5)

    @pl.when(end)
    def _():
        pl.semaphore_wait(barrier, 4)

    @pl.loop(0, NS)
    def _(i):
        transpose(i)

    steps = {1: stage1, 2: stage2, 3: stage3, 4: stage4, 5: stage5, 6: stage6, 7: stage7, 8: stage8,
             "A": stage_a, "B": stage_b, "M0": matmul0, "M1": matmul1}

    @pl.loop(0, NC + max(OFF.values()))
    def _(t):
        for name in ORDER:
            steps[name](t - OFF.get(name, 0))

    for c in range(NC - LAG, NC):
        for where, copies in sent:
            @pl.when(where)
            def _():
                for copy in copies:
                    for ab in range(2):
                        copy(c, ab).wait_send()
        d_copy(c, other).wait_send()
        ce(c, mine).wait_send()

    @pl.loop(0, NC)
    def _(c):
        ce(c, other).wait_recv()


def place_kernel(res, out, sem):
    def copy(i):
        c, ab = i // 2, i % 2
        cols = pl.ds(pl.multiple_of((c % PER) * W + ab * 128, 128), 128)
        return pltpu.make_async_copy(res.at[c, ab], out.at[c // PER, :, cols], sem)

    @pl.loop(0, 2 * NC)
    def _(i):
        copy(i).start()

    pltpu.make_async_copy(res, res, sem).wait()


def total(a, g):
    res = pl.pallas_call(
        kernel,
        out_shape=pltpu.VMEM((NC, 2, D, 128), BF),
        in_specs=[pl.BlockSpec(memory_space=pl.ANY)] * 2,
        out_specs=pl.BlockSpec(memory_space=pltpu.VMEM),
        scratch_shapes=list(SCRATCH.values()),
        compiler_params=pltpu.CompilerParams(
            collective_id=0, has_side_effects=True, vmem_limit_bytes=42 * 2**20),
        name="sum_tiles",
    )(a, g)
    return pl.pallas_call(
        place_kernel,
        out_shape=jax.ShapeDtypeStruct((N, D, FF), BF),
        in_specs=[pl.BlockSpec(memory_space=pltpu.VMEM)],
        out_specs=pl.BlockSpec(memory_space=pl.ANY),
        scratch_shapes=[pltpu.SemaphoreType.DMA],
        compiler_params=pltpu.CompilerParams(vmem_limit_bytes=30 * 2**20),
        name="place",
    )(res)


def solution(mesh):
    def body(a, g):
        return total(a[0], g[0])

    return jax.shard_map(body, mesh=mesh, in_specs=(P(("rep", "dp")), P(("rep", "dp"))),
                         out_specs=P("rep"), check_vma=False)
```
